128 devices in a mesh: ty: 8 (over x, core), tx: 16 (over y, z).
Axes of the slice: x: 4, y: 4, z: 4, core: 2. Of those that a mesh axis runs over, the one named last changes fastest.
Arguments:
- intensity: float32 [256, 256, 256], P(('ty', 'tx')), may hold values from 0 to 3
- corner: int32 [256, 2], P(('ty', 'tx')), may hold values from 0 to 1792, as said below
- probe: float32 [2, 256, 256], replicated, may hold values from -6 to 6
- prop_phase: float32 [256, 256], replicated, may hold values from -3.140625 to 3.140625
- object_slices: float32 [2, 2, 2048, 2048], P(None, None, 'ty', 'tx'), may hold values from -5 to 5
- momentum: float32 [2, 2, 2048, 2048], P(None, None, 'ty', 'tx'), may hold values from -6 to 6
Outputs:
- object_next: float32 [2, 2, 2048, 2048], P(None, None, 'ty', 'tx')
- momentum_next: float32 [2, 2, 2048, 2048], P(None, None, 'ty', 'tx')
The draws below stay inside these ranges and needn't reach their ends.
Inputs may be any that keep to these rules, and one draw needn't show every extreme that they name: `corner`: patch p belongs to device p // 2 of ty+tx (ty slowest); with t = p // (2 times the size of tx) and s = (p // 2) modulo the size of tx, its row offset lies between max(t * 256 - 256 / 2, 0) and min(t * 256 + 256 - 256 / 2, 1792), and its column offset between max(s * 128 - 256 / 2, 0) and min(s * 128 + 128 - 256 / 2, 1792).
All inputs are finite; a program needn't handle non-finite values.
Results may differ from the reference program's by a relative error of at most 0.0003.
Values sent between devices are 32-bit elements; how exact they have to be, the bound alone decides.
No kernel may reach another device: no remote copies, remote signals or barrier semaphores. Data moves between devices by JAX's collectives and lax.ppermute only.
A program may use at most 64 MiB of HBM per device.

```python
import jax
import jax.numpy as jnp
from jax import lax

PATCH = 256
PAT_DEV = 2
TILE_Y = 256
TILE_X = 128
PATCHES = 256
OY = 2048
OX = 2048
N_TX = 16


def draw_corner(key, part):
    member = jnp.arange(PATCHES, dtype=jnp.int32)
    tile_row = member // (PAT_DEV * N_TX)
    tile_col = member // PAT_DEV % N_TX
    row_low = jnp.maximum(tile_row * TILE_Y - PATCH // 2, 0)
    row_high = jnp.minimum(tile_row * TILE_Y + TILE_Y - PATCH // 2, OY - PATCH)
    col_low = jnp.maximum(tile_col * TILE_X - PATCH // 2, 0)
    col_high = jnp.minimum(tile_col * TILE_X + TILE_X - PATCH // 2, OX - PATCH)
    row_key, col_key = jax.random.split(jax.random.fold_in(key, 7))
    row_start = jax.random.randint(row_key, (PATCHES,), row_low, row_high + 1)
    col_start = jax.random.randint(col_key, (PATCHES,), col_low, col_high + 1)
    return jnp.stack([row_start, col_start], axis=1).astype(jnp.int32)


def level_of(own_key, extent, cuts, smallest, top_value):
    def one(dim, blocks):
        steps = jax.random.uniform(jax.random.fold_in(jax.random.fold_in(own_key, 6), dim), (blocks,), jnp.float32, smallest / len(cuts), top_value / len(cuts))
        return jnp.repeat(jnp.exp(steps), extent[dim] // blocks).reshape((-1,) + (1,) * (len(extent) - dim - 1))

    level = one(*cuts[0])
    for cut in cuts[1:]:
        level = level * one(*cut)
    return level


def normal_values(key, extent, deviation, bound, cuts=(), kind=jnp.bfloat16):
    result = deviation * jax.random.normal(key, extent, jnp.float32)
    if cuts:
        result = result * level_of(key, extent, cuts, -0.22, 0.18)
    return jnp.clip(result, -bound, bound).astype(kind)


def setup_inputs(seed: int = 0) -> dict:
    streams_of = jax.random.split(jax.random.key(seed), 7)
    intensity = jnp.clip(3.0 * jax.random.uniform(streams_of[0], (PATCHES, PATCH, PATCH), jnp.float32) ** level_of(streams_of[0], (PATCHES, PATCH, PATCH), ((0, 128),), -0.2, 0.2), 0.0, 3.0)
    corner = draw_corner(jax.random.fold_in(streams_of[6], 71), 0)
    probe = normal_values(streams_of[2], (2, PATCH, PATCH), 1.0, 6.0, (), jnp.float32)
    prop_phase = jnp.clip(jax.random.uniform(streams_of[3], (PATCH, PATCH), jnp.float32, -3.140625, 3.140625), -3.140625, 3.140625)
    object_slices = normal_values(streams_of[4], (2, 2, OY, OX), 0.7, 5.0, ((2, 8), (3, 16)), jnp.float32)
    momentum = normal_values(streams_of[5], (2, 2, OY, OX), 1.0, 6.0, ((2, 8), (3, 16)), jnp.float32)
    return dict(intensity=intensity, corner=corner, probe=probe, prop_phase=prop_phase, object_slices=object_slices, momentum=momentum)


decay_rate = 0.9
grad_scale = 0.05
step_length = 0.5


def forward(field):
    return jnp.fft.fft2(field, norm="ortho")


def inverse(field):
    return jnp.fft.ifft2(field, norm="ortho")


def reference(intensity, corner, probe, prop_phase, object_slices, momentum):
    probe_wave = lax.complex(probe[0], probe[1])
    transfer = lax.complex(jnp.cos(prop_phase), jnp.sin(prop_phase))
    objects = lax.complex(object_slices[:, 0], object_slices[:, 1])

    def accumulate(gradient, packed):
        offsets, measured = packed
        start = (jnp.zeros((), jnp.int32), offsets[0].astype(jnp.int32), offsets[1].astype(jnp.int32))
        window = lax.dynamic_slice(objects, start, (2, PATCH, PATCH))
        exit_wave = inverse(transfer * forward(probe_wave * window[0]))
        far_field = forward(exit_wave * window[1])
        residue = far_field.real ** 2 + far_field.imag ** 2 - measured
        back_wave = inverse(2.0 * residue * far_field)
        second = jnp.conj(exit_wave) * back_wave
        first = jnp.conj(probe_wave) * inverse(jnp.conj(transfer) * forward(jnp.conj(window[1]) * back_wave))
        current = lax.dynamic_slice(gradient, start, (2, PATCH, PATCH))
        return lax.dynamic_update_slice(gradient, current + jnp.stack([first, second]), start), None

    gradient, unused = lax.scan(accumulate, jnp.zeros_like(objects), (corner, intensity))
    grad_parts = jnp.stack([gradient.real, gradient.imag], axis=1)
    momentum_next = decay_rate * momentum + grad_scale * grad_parts
    object_next = object_slices - step_length * momentum_next
    return object_next, momentum_next
```

```python
import functools
import math

import jax
import jax.numpy as jnp
import numpy as np
from jax import lax
from jax.experimental import pallas as pl
from jax.experimental.pallas import tpu as pltpu
from jax.sharding import PartitionSpec as P

decay_rate = 0.9
grad_scale = 0.05
step_length = 0.5

N = 256
HALF = 128
bf16 = jnp.bfloat16
f32 = jnp.float32


def dft_tables():
    j = np.arange(HALF)[:, None]
    k = np.arange(HALF)[None, :]
    even = np.exp(-2j * math.pi * (j * (2 * k) % N) / N) / math.sqrt(N)
    odd = np.exp(-2j * math.pi * (j * (2 * k + 1) % N) / N) / math.sqrt(N)
    out = []
    for m in (even, odd):
        real = np.block([[m.real, m.imag], [-m.imag, m.real]])
        for t in (real, real.T):
            t = t.astype(np.float32)
            hi = t.astype(jnp.bfloat16)
            lo = (t - hi.astype(np.float32)).astype(jnp.bfloat16)
            out += [hi, lo]
    return np.stack(out)


EVEN, EVEN_T, ODD, ODD_T = (0, 2, 4, 6)


def split(x):
    hi = x.astype(bf16)
    lo = (x - hi.astype(f32)).astype(bf16)
    return hi, lo


def dot(a, b):
    return jnp.dot(a, b, preferred_element_type=f32)


def left_mul(tab, which, x):
    hi, lo = split(x)
    return dot(tab[which], hi) + dot(tab[which], lo) + dot(tab[which + 1], hi)


def right_mul(tab, which, x):
    hi, lo = split(x)
    return dot(hi, tab[which]) + dot(lo, tab[which]) + dot(hi, tab[which + 1])


def cat(parts, axis):
    return jnp.concatenate(parts, axis=axis)


def forward(tab, re, im):
    a = cat([re[:HALF] + re[HALF:], im[:HALF] + im[HALF:]], 0)
    b = cat([re[:HALF] - re[HALF:], im[:HALF] - im[HALF:]], 0)
    e = left_mul(tab, EVEN_T, a)
    o = left_mul(tab, ODD_T, b)
    re = cat([e[:HALF], o[:HALF]], 0)
    im = cat([e[HALF:], o[HALF:]], 0)
    a = cat([re[:, :HALF] + re[:, HALF:], im[:, :HALF] + im[:, HALF:]], 1)
    b = cat([re[:, :HALF] - re[:, HALF:], im[:, :HALF] - im[:, HALF:]], 1)
    e = right_mul(tab, EVEN, a)
    o = right_mul(tab, ODD, b)
    re = cat([e[:, :HALF], o[:, :HALF]], 1)
    im = cat([e[:, HALF:], o[:, HALF:]], 1)
    return re, im


def inverse(tab, re, im):
    e = right_mul(tab, EVEN_T, cat([re[:, :HALF], im[:, :HALF]], 1))
    o = right_mul(tab, ODD_T, cat([re[:, HALF:], im[:, HALF:]], 1))
    s, d = e + o, e - o
    re = cat([s[:, :HALF], d[:, :HALF]], 1)
    im = cat([s[:, HALF:], d[:, HALF:]], 1)
    e = left_mul(tab, EVEN, cat([re[:HALF], im[:HALF]], 0))
    o = left_mul(tab, ODD, cat([re[HALF:], im[HALF:]], 0))
    s, d = e + o, e - o
    re = cat([s[:HALF], d[:HALF]], 0)
    im = cat([s[HALF:], d[HALF:]], 0)
    return re, im


def cmul(ar, ai, br, bi):
    return ar * br - ai * bi, ar * bi + ai * br


def cmul_conj(ar, ai, br, bi):
    return ar * br + ai * bi, ar * bi - ai * br


def masks(pos, p):
    row = pos[p, 0]
    col = pos[p, 1]
    i = lax.broadcasted_iota(jnp.int32, (HALF, HALF), 0)
    j = lax.broadcasted_iota(jnp.int32, (HALF, HALF), 1)
    return i >= row, i + HALF >= row, j >= col


def window(own, left, right, up, down, pos, p, c):
    top, bottom, near = masks(pos, p)
    side_u = jnp.where(near, up[c, :, :HALF], up[c, :, N:])
    side_d = jnp.where(near, down[c, :, :HALF], down[c, :, N:])
    side_o = jnp.where(cat([near, near], 0), left[c], right[c])
    side = cat([jnp.where(top, side_u, side_o[HALF:]), jnp.where(bottom, side_o[:HALF], side_d)], 0)
    mid = cat(
        [
            jnp.where(top, up[c, :, HALF:N], own[c, HALF:, :]),
            jnp.where(bottom, own[c, :HALF, :], down[c, :, HALF:N]),
        ],
        0,
    )
    return cat([side, mid], 1)


def put_gradient(g0, g1, c, pos, own, left, right, up, down):
    def pieces(g, p):
        top, bottom, near = masks(pos, p)
        zero = jnp.zeros((HALF, HALF), f32)
        out = []
        for rows, keep in ((g[:HALF], top), (g[HALF:], bottom)):
            for inside in (keep, jnp.logical_not(keep)):
                side = jnp.where(inside, rows[:, :HALF], zero)
                mid = jnp.where(inside, rows[:, HALF:], zero)
                out.append((jnp.where(near, side, zero), mid, jnp.where(near, zero, side)))
        return out

    u0, b0, t0, d0 = pieces(g0, 0)
    u1, b1, t1, d1 = pieces(g1, 1)
    for k in range(3):
        cols = slice(k * HALF, (k + 1) * HALF)
        up[c, :, cols] = u0[k] + u1[k]
        down[c, :, cols] = d0[k] + d1[k]
        part = (left, own, right)[k]
        part[c, :HALF, :] = t0[k] + t1[k]
        part[c, HALF:, :] = b0[k] + b1[k]


def prepare_kernel(pos, probe, phase, intensity, probe_out, trans_out, intensity_out):
    for p in range(2):
        row = pos[p, 0]
        col = pos[p, 1]
        for c in range(2):
            rolled = pltpu.roll(probe[c], row, 0)
            probe_out[p, c] = pltpu.roll(rolled, col, 1)
    i = lax.broadcasted_iota(jnp.int32, (N, N), 0)
    j = lax.broadcasted_iota(jnp.int32, (N, N), 1)
    source = jnp.where(j < HALF, 2 * j, 2 * (j - HALF) + 1)
    pick = jnp.where(i == source, 1.0, 0.0).astype(bf16)
    target = jnp.where(i < HALF, 2 * i, 2 * (i - HALF) + 1)
    pick_rows = jnp.where(j == target, 1.0, 0.0).astype(bf16)

    def thirds(x):
        hi = x.astype(bf16)
        rest = x - hi.astype(f32)
        mid = rest.astype(bf16)
        return hi, mid, (rest - mid.astype(f32)).astype(bf16)

    def reorder(x):
        x = sum(dot(pick_rows, part) for part in thirds(x))
        return sum(dot(part, pick) for part in thirds(x))

    ph = reorder(phase[...])
    trans_out[0] = jnp.cos(ph)
    trans_out[1] = jnp.sin(ph)
    for p in range(2):
        intensity_out[p] = reorder(intensity[p])


def exit_kernel(pos, own, left, right, up, down, probe, trans, tab, wave):
    for p in range(2):
        wr = window(own, left, right, up, down, pos, p, 0)
        wi = window(own, left, right, up, down, pos, p, 1)
        re, im = cmul(probe[p, 0], probe[p, 1], wr, wi)
        re, im = forward(tab, re, im)
        re, im = cmul(trans[0], trans[1], re, im)
        re, im = inverse(tab, re, im)
        wave[p, 0] = re
        wave[p, 1] = im


def far_kernel(pos, own, left, right, up, down, wave, intensity, tab, back, g_own, g_left, g_right, g_up, g_down):
    grads = []
    for p in range(2):
        wr = window(own, left, right, up, down, pos, p, 0)
        wi = window(own, left, right, up, down, pos, p, 1)
        re, im = cmul(wave[p, 0], wave[p, 1], wr, wi)
        re, im = forward(tab, re, im)
        scale = 2.0 * (re * re + im * im - intensity[p])
        re, im = inverse(tab, scale * re, scale * im)
        br, bi = cmul_conj(wr, wi, re, im)
        back[p, 0] = br
        back[p, 1] = bi
        grads.append(cmul_conj(wave[p, 0], wave[p, 1], re, im))
    for c in range(2):
        put_gradient(grads[0][c], grads[1][c], c, pos, g_own, g_left, g_right, g_up, g_down)


def first_kernel(pos, back, probe, trans, tab, g_own, g_left, g_right, g_up, g_down):
    grads = []
    for p in range(2):
        re, im = forward(tab, back[p, 0], back[p, 1])
        re, im = cmul_conj(trans[0], trans[1], re, im)
        re, im = inverse(tab, re, im)
        grads.append(cmul_conj(probe[p, 0], probe[p, 1], re, im))
    for c in range(2):
        put_gradient(grads[0][c], grads[1][c], c, pos, g_own, g_left, g_right, g_up, g_down)


def call(kernel, outs, args, flops, name):
    specs = [pl.BlockSpec(memory_space=pltpu.SMEM)] + [pl.BlockSpec(memory_space=pltpu.VMEM)] * (len(args) - 1)
    return pl.pallas_call(
        kernel,
        out_shape=[jax.ShapeDtypeStruct(s, f32) for s in outs],
        in_specs=specs,
        out_specs=[pl.BlockSpec(memory_space=pltpu.VMEM)] * len(outs),
        compiler_params=pltpu.CompilerParams(vmem_limit_bytes=20 * 2**20),
        cost_estimate=pl.CostEstimate(flops=flops, bytes_accessed=4 * 2**20, transcendentals=0),
        name=name,
    )(*args)


GRAD_SHAPES = ((2, 256, 128),) * 3 + ((2, 128, 384),) * 2


def pairs(axis, steps):
    count = lax.axis_size(axis)
    return [(s, s + steps) for s in range(count) if 0 <= s + steps < count]


def shifted(value, axis, steps):
    return lax.ppermute(value, axis, pairs(axis, steps))


def halos(tile):
    left = shifted(tile, "tx", 1)
    right = shifted(tile, "tx", -1)
    band = cat([left, tile, right], 2)
    up = shifted(band[:, HALF:], "ty", 1)
    down = shifted(band[:, :HALF], "ty", -1)
    return tile, left, right, up, down


def gather_gradient(own, left, right, up, down):
    below = shifted(up, "ty", -1)
    above = shifted(down, "ty", 1)
    both = cat([above, below], 1)
    from_right = shifted(left + both[:, :, :HALF], "tx", -1)
    from_left = shifted(right + both[:, :, N:], "tx", 1)
    return own + both[:, :, HALF:N] + from_right + from_left


def on_device(intensity, corner, probe, prop_phase, object_slices, momentum):
    tile_rows, tile_cols = object_slices.shape[2:]
    origin = jnp.stack(
        [lax.axis_index("ty") * tile_rows - HALF, lax.axis_index("tx") * tile_cols - HALF]
    )
    pos = corner - origin[None, :]
    tab = jnp.asarray(dft_tables())
    probe_r, trans, inten = call(
        prepare_kernel,
        ((2, 2, N, N), (2, N, N), (2, N, N)),
        (pos, probe, prop_phase, intensity),
        2 * 10**9,
        "prepare",
    )
    first = halos(object_slices[0])
    second = halos(object_slices[1])
    (wave,) = call(exit_kernel, ((2, 2, N, N),), (pos, *first, probe_r, trans, tab), 4 * 10**9, "exit_wave")
    back, *g2 = call(
        far_kernel, ((2, 2, N, N),) + GRAD_SHAPES, (pos, *second, wave, inten, tab), 4 * 10**9, "far_wave"
    )
    g1 = call(first_kernel, GRAD_SHAPES, (pos, back, probe_r, trans, tab), 4 * 10**9, "first_wave")
    grad_second = gather_gradient(*g2)
    grad_first = gather_gradient(*g1)
    gradient = jnp.stack([grad_first, grad_second])
    momentum_next = decay_rate * momentum + grad_scale * gradient
    object_next = object_slices - step_length * momentum_next
    return (object_next, momentum_next)


def solution(mesh):
    return jax.shard_map(
        on_device,
        mesh=mesh,
        in_specs=(
            P(("ty", "tx"), None, None),
            P(("ty", "tx"), None),
            P(),
            P(),
            P(None, None, "ty", "tx"),
            P(None, None, "ty", "tx"),
        ),
        out_specs=(P(None, None, "ty", "tx"), P(None, None, "ty", "tx")),
        check_vma=False,
    )
```

```python
import math

import jax
import jax.numpy as jnp
import numpy as np
from jax import lax
from jax.experimental import pallas as pl
from jax.experimental.pallas import tpu as pltpu
from jax.sharding import PartitionSpec as P


decay_rate = 0.9
grad_scale = 0.05
step_length = 0.5

N = 256
HALF = 128
bf16 = jnp.bfloat16
f32 = jnp.float32


def dft_tables():
    j = np.arange(HALF)[:, None]
    k = np.arange(HALF)[None, :]
    even = np.exp(-2j * math.pi * (j * (2 * k) % N) / N) / math.sqrt(N)
    odd = np.exp(-2j * math.pi * (j * (2 * k + 1) % N) / N) / math.sqrt(N)
    out = []
    for m in (even, odd):
        real = np.block([[m.real, m.imag], [-m.imag, m.real]])
        for t in (real, real.T):
            t = t.astype(np.float32)
            hi = t.astype(jnp.bfloat16)
            lo = (t - hi.astype(np.float32)).astype(jnp.bfloat16)
            out += [hi, lo]
    return np.stack(out)


EVEN, EVEN_T, ODD, ODD_T = (0, 2, 4, 6)


def split(x):
    hi = x.astype(bf16)
    lo = (x - hi.astype(f32)).astype(bf16)
    return hi, lo


def dot(a, b):
    return jnp.dot(a, b, preferred_element_type=f32)


def left_mul(tab, which, x):
    hi, lo = split(x)
    return dot(tab[which], hi) + dot(tab[which], lo) + dot(tab[which + 1], hi)


def right_mul(tab, which, x):
    hi, lo = split(x)
    return dot(hi, tab[which]) + dot(lo, tab[which]) + dot(hi, tab[which + 1])


def cat(parts, axis):
    return jnp.concatenate(parts, axis=axis)


def forward(tab, re, im):
    a = cat([re[:HALF] + re[HALF:], im[:HALF] + im[HALF:]], 0)
    b = cat([re[:HALF] - re[HALF:], im[:HALF] - im[HALF:]], 0)
    e = left_mul(tab, EVEN_T, a)
    o = left_mul(tab, ODD_T, b)
    re = cat([e[:HALF], o[:HALF]], 0)
    im = cat([e[HALF:], o[HALF:]], 0)
    a = cat([re[:, :HALF] + re[:, HALF:], im[:, :HALF] + im[:, HALF:]], 1)
    b = cat([re[:, :HALF] - re[:, HALF:], im[:, :HALF] - im[:, HALF:]], 1)
    e = right_mul(tab, EVEN, a)
    o = right_mul(tab, ODD, b)
    re = cat([e[:, :HALF], o[:, :HALF]], 1)
    im = cat([e[:, HALF:], o[:, HALF:]], 1)
    return re, im


def inverse(tab, re, im):
    e = right_mul(tab, EVEN_T, cat([re[:, :HALF], im[:, :HALF]], 1))
    o = right_mul(tab, ODD_T, cat([re[:, HALF:], im[:, HALF:]], 1))
    s, d = e + o, e - o
    re = cat([s[:, :HALF], d[:, :HALF]], 1)
    im = cat([s[:, HALF:], d[:, HALF:]], 1)
    e = left_mul(tab, EVEN, cat([re[:HALF], im[:HALF]], 0))
    o = left_mul(tab, ODD, cat([re[HALF:], im[HALF:]], 0))
    s, d = e + o, e - o
    re = cat([s[:HALF], d[:HALF]], 0)
    im = cat([s[HALF:], d[HALF:]], 0)
    return re, im


def cmul(ar, ai, br, bi):
    return ar * br - ai * bi, ar * bi + ai * br


def cmul_conj(ar, ai, br, bi):
    return ar * br + ai * bi, ar * bi - ai * br


def masks(pos, p):
    row = pos[p, 0]
    col = pos[p, 1]
    i = lax.broadcasted_iota(jnp.int32, (HALF, HALF), 0)
    j = lax.broadcasted_iota(jnp.int32, (HALF, HALF), 1)
    flip = jnp.full((HALF, HALF), pos[2, 1]) == 1
    low = jnp.full((HALF, HALF), pos[2, 0]) == 1
    return i >= row, i + HALF >= row, (j >= col) == flip, low


def pick_rows(low, a, b):
    return jnp.where(low, a, b), jnp.where(low, b, a)


def window(own, cols_a, cols_b, rows_a, rows_b, pos, p, c):
    top, bottom, near, low = masks(pos, p)

    def band(k):
        return pick_rows(low, rows_a[c, :, k * HALF : (k + 1) * HALF], rows_b[c, :, k * HALF : (k + 1) * HALF])

    (up_a, down_a), (up, down), (up_b, down_b) = (band(0), band(1), band(2))
    side_u = jnp.where(near, up_a, up_b)
    side_d = jnp.where(near, down_a, down_b)
    side_t = jnp.where(near, cols_a[c, :HALF], cols_b[c, :HALF])
    side_l = jnp.where(near, cols_a[c, HALF:], cols_b[c, HALF:])
    side = cat([jnp.where(top, side_u, side_l), jnp.where(bottom, side_t, side_d)], 0)
    mid = cat([jnp.where(top, up, own[c, HALF:, :]), jnp.where(bottom, own[c, :HALF, :], down)], 0)
    return cat([side, mid], 1)


def put_gradient(g0, g1, c, pos, own, cols_a, cols_b, rows_a, rows_b):
    def pieces(g, p):
        top, bottom, near, _ = masks(pos, p)
        zero = jnp.zeros((HALF, HALF), f32)
        out = []
        for rows, keep in ((g[:HALF], top), (g[HALF:], bottom)):
            for inside in (keep, jnp.logical_not(keep)):
                side = jnp.where(inside, rows[:, :HALF], zero)
                mid = jnp.where(inside, rows[:, HALF:], zero)
                out.append((jnp.where(near, side, zero), mid, jnp.where(near, zero, side)))
        return out

    low = masks(pos, 0)[3]
    u0, b0, t0, d0 = pieces(g0, 0)
    u1, b1, t1, d1 = pieces(g1, 1)
    for k in range(3):
        cols = slice(k * HALF, (k + 1) * HALF)
        first, second = pick_rows(low, u0[k] + u1[k], d0[k] + d1[k])
        rows_a[c, :, cols] = first
        rows_b[c, :, cols] = second
        part = (cols_a, own, cols_b)[k]
        part[c, :HALF, :] = t0[k] + t1[k]
        part[c, HALF:, :] = b0[k] + b1[k]


def prepare_kernel(pos, probe, phase, intensity, probe_out, trans_out, intensity_out):
    for p in range(2):
        row = pos[p, 0]
        col = pos[p, 1]
        for c in range(2):
            rolled = pltpu.roll(probe[c], row, 0)
            probe_out[p, c] = pltpu.roll(rolled, col, 1)
    i = lax.broadcasted_iota(jnp.int32, (N, N), 0)
    j = lax.broadcasted_iota(jnp.int32, (N, N), 1)
    source = jnp.where(j < HALF, 2 * j, 2 * (j - HALF) + 1)
    pick = jnp.where(i == source, 1.0, 0.0).astype(bf16)
    target = jnp.where(i < HALF, 2 * i, 2 * (i - HALF) + 1)
    pick_rows = jnp.where(j == target, 1.0, 0.0).astype(bf16)

    def thirds(x):
        hi = x.astype(bf16)
        rest = x - hi.astype(f32)
        mid = rest.astype(bf16)
        return hi, mid, (rest - mid.astype(f32)).astype(bf16)

    def reorder(x):
        x = sum(dot(pick_rows, part) for part in thirds(x))
        return sum(dot(part, pick) for part in thirds(x))

    ph = reorder(phase[...])
    trans_out[0] = jnp.cos(ph)
    trans_out[1] = jnp.sin(ph)
    for p in range(2):
        intensity_out[p] = reorder(intensity[p])


def exit_kernel(pos, own, cols_a, cols_b, rows_a, rows_b, probe, trans, tab, wave):
    for p in range(2):
        wr = window(own, cols_a, cols_b, rows_a, rows_b, pos, p, 0)
        wi = window(own, cols_a, cols_b, rows_a, rows_b, pos, p, 1)
        re, im = cmul(probe[p, 0], probe[p, 1], wr, wi)
        re, im = forward(tab, re, im)
        re, im = cmul(trans[0], trans[1], re, im)
        re, im = inverse(tab, re, im)
        wave[p, 0] = re
        wave[p, 1] = im


def far_kernel(pos, own, cols_a, cols_b, rows_a, rows_b, wave, intensity, tab, back, g_own, g_cols_a, g_cols_b, g_rows_a, g_rows_b):
    grads = []
    for p in range(2):
        wr = window(own, cols_a, cols_b, rows_a, rows_b, pos, p, 0)
        wi = window(own, cols_a, cols_b, rows_a, rows_b, pos, p, 1)
        re, im = cmul(wave[p, 0], wave[p, 1], wr, wi)
        re, im = forward(tab, re, im)
        scale = 2.0 * (re * re + im * im - intensity[p])
        re, im = inverse(tab, scale * re, scale * im)
        br, bi = cmul_conj(wr, wi, re, im)
        back[p, 0] = br
        back[p, 1] = bi
        grads.append(cmul_conj(wave[p, 0], wave[p, 1], re, im))
    for c in range(2):
        put_gradient(grads[0][c], grads[1][c], c, pos, g_own, g_cols_a, g_cols_b, g_rows_a, g_rows_b)


def first_kernel(pos, back, probe, trans, tab, g_own, g_cols_a, g_cols_b, g_rows_a, g_rows_b):
    grads = []
    for p in range(2):
        re, im = forward(tab, back[p, 0], back[p, 1])
        re, im = cmul_conj(trans[0], trans[1], re, im)
        re, im = inverse(tab, re, im)
        grads.append(cmul_conj(probe[p, 0], probe[p, 1], re, im))
    for c in range(2):
        put_gradient(grads[0][c], grads[1][c], c, pos, g_own, g_cols_a, g_cols_b, g_rows_a, g_rows_b)


def call(kernel, outs, args, flops):
    specs = [pl.BlockSpec(memory_space=pltpu.SMEM)] + [pl.BlockSpec(memory_space=pltpu.VMEM)] * (len(args) - 1)
    return pl.pallas_call(
        kernel,
        out_shape=[jax.ShapeDtypeStruct(s, f32) for s in outs],
        in_specs=specs,
        out_specs=[pl.BlockSpec(memory_space=pltpu.VMEM)] * len(outs),
        compiler_params=pltpu.CompilerParams(vmem_limit_bytes=20 * 2**20),
        cost_estimate=pl.CostEstimate(flops=flops, bytes_accessed=4 * 2**20, transcendentals=0),
    )(*args)


GRAD_SHAPES = ((2, 256, 128),) * 3 + ((2, 128, 384),) * 2


def swap(value, axis, first):
    count = lax.axis_size(axis)
    there = [(k, k + 1) for k in range(first, count - 1, 2)]
    return lax.ppermute(value, axis, there + [(b, a) for a, b in there])


def halos(tile, low):
    cols_b = swap(tile, "tx", 1)
    cols_a = swap(tile, "tx", 0)
    band = cat([cols_a, tile, cols_b], 2)
    top, bottom = (band[:, :HALF], band[:, HALF:])
    rows_b = swap(jnp.where(low, bottom, top), "ty", 1)
    rows_a = swap(jnp.where(low, top, bottom), "ty", 0)
    return tile, cols_a, cols_b, rows_a, rows_b


def gather_gradient(low, own, cols_a, cols_b, rows_a, rows_b):
    rows_b = swap(rows_b, "ty", 1)
    rows_a = swap(rows_a, "ty", 0)
    top, bottom = (jnp.where(low, rows_a, rows_b), jnp.where(low, rows_b, rows_a))

    def merged(part, k):
        cols = slice(k * HALF, (k + 1) * HALF)
        return cat([part[:, :HALF] + top[:, :, cols], part[:, HALF:] + bottom[:, :, cols]], 1)

    send_a, send_b = merged(cols_a, 0), merged(cols_b, 2)
    from_b = swap(send_b, "tx", 1)
    from_a = swap(send_a, "tx", 0)
    return merged(own, 1) + from_a + from_b


def on_device(intensity, corner, probe, prop_phase, object_slices, momentum):
    tile_rows, tile_cols = object_slices.shape[2:]
    at_y, at_x = (lax.axis_index("ty"), lax.axis_index("tx"))
    origin = jnp.stack([at_y * tile_rows - HALF, at_x * tile_cols - HALF])
    parity = jnp.stack([at_y % 2, at_x % 2])
    pos = jnp.concatenate([corner - origin[None, :], parity[None, :]])
    low = at_y % 2 == 1
    tab = jnp.asarray(dft_tables())
    first = halos(object_slices[0], low)
    second = halos(object_slices[1], low)
    probe_r, trans, inten = call(
        prepare_kernel, ((2, 2, N, N), (2, N, N), (2, N, N)), (pos, probe, prop_phase, intensity), 2 * 10**9
    )
    (wave,) = call(exit_kernel, ((2, 2, N, N),), (pos, *first, probe_r, trans, tab), 4 * 10**9)
    back, *g2 = call(far_kernel, ((2, 2, N, N),) + GRAD_SHAPES, (pos, *second, wave, inten, tab), 4 * 10**9)
    g1 = call(first_kernel, GRAD_SHAPES, (pos, back, probe_r, trans, tab), 4 * 10**9)
    grad_second = gather_gradient(low, *g2)
    grad_first = gather_gradient(low, *g1)
    gradient = jnp.stack([grad_first, grad_second])
    momentum_next = decay_rate * momentum + grad_scale * gradient
    object_next = object_slices - step_length * momentum_next
    return (object_next, momentum_next)


def solution(mesh):
    return jax.shard_map(
        on_device,
        mesh=mesh,
        in_specs=(
            P(("ty", "tx"), None, None),
            P(("ty", "tx"), None),
            P(),
            P(),
            P(None, None, "ty", "tx"),
            P(None, None, "ty", "tx"),
        ),
        out_specs=(P(None, None, "ty", "tx"), P(None, None, "ty", "tx")),
        check_vma=False,
    )
```

```python
import math

import jax
import jax.numpy as jnp
import numpy as np
from jax import lax
from jax.experimental import pallas as pl
from jax.experimental.pallas import tpu as pltpu
from jax.sharding import PartitionSpec as P


decay_rate = 0.9
grad_scale = 0.05
step_length = 0.5

N = 256
HALF = 128
bf16 = jnp.bfloat16
f32 = jnp.float32


def dft_tables():
    j = np.arange(HALF)[:, None]
    k = np.arange(HALF)[None, :]
    even = np.exp(-2j * math.pi * (j * (2 * k) % N) / N) / math.sqrt(N)
    odd = np.exp(-2j * math.pi * (j * (2 * k + 1) % N) / N) / math.sqrt(N)
    out = []
    for m in (even, odd):
        real = np.block([[m.real, m.imag], [-m.imag, m.real]])
        for t in (real, real.T):
            t = t.astype(np.float32)
            hi = t.astype(jnp.bfloat16)
            lo = (t - hi.astype(np.float32)).astype(jnp.bfloat16)
            out += [hi, lo]
    return np.stack(out)


EVEN, EVEN_T, ODD, ODD_T = (0, 2, 4, 6)


def split(x):
    hi = x.astype(bf16)
    lo = (x - hi.astype(f32)).astype(bf16)
    return hi, lo


def dot(a, b):
    return jnp.dot(a, b, preferred_element_type=f32)


def left_mul(tab, which, x):
    hi, lo = split(x)
    return dot(tab[which], hi) + dot(tab[which], lo) + dot(tab[which + 1], hi)


def right_mul(tab, which, x):
    hi, lo = split(x)
    return dot(hi, tab[which]) + dot(lo, tab[which]) + dot(hi, tab[which + 1])


def cat(parts, axis):
    return jnp.concatenate(parts, axis=axis)


def forward(tab, re, im):
    a = cat([re[:HALF] + re[HALF:], im[:HALF] + im[HALF:]], 0)
    b = cat([re[:HALF] - re[HALF:], im[:HALF] - im[HALF:]], 0)
    e = left_mul(tab, EVEN_T, a)
    o = left_mul(tab, ODD_T, b)
    re = cat([e[:HALF], o[:HALF]], 0)
    im = cat([e[HALF:], o[HALF:]], 0)
    a = cat([re[:, :HALF] + re[:, HALF:], im[:, :HALF] + im[:, HALF:]], 1)
    b = cat([re[:, :HALF] - re[:, HALF:], im[:, :HALF] - im[:, HALF:]], 1)
    e = right_mul(tab, EVEN, a)
    o = right_mul(tab, ODD, b)
    re = cat([e[:, :HALF], o[:, :HALF]], 1)
    im = cat([e[:, HALF:], o[:, HALF:]], 1)
    return re, im


def inverse(tab, re, im):
    e = right_mul(tab, EVEN_T, cat([re[:, :HALF], im[:, :HALF]], 1))
    o = right_mul(tab, ODD_T, cat([re[:, HALF:], im[:, HALF:]], 1))
    s, d = e + o, e - o
    re = cat([s[:, :HALF], d[:, :HALF]], 1)
    im = cat([s[:, HALF:], d[:, HALF:]], 1)
    e = left_mul(tab, EVEN, cat([re[:HALF], im[:HALF]], 0))
    o = left_mul(tab, ODD, cat([re[HALF:], im[HALF:]], 0))
    s, d = e + o, e - o
    re = cat([s[:HALF], d[:HALF]], 0)
    im = cat([s[HALF:], d[HALF:]], 0)
    return re, im


def cmul(ar, ai, br, bi):
    return ar * br - ai * bi, ar * bi + ai * br


def cmul_conj(ar, ai, br, bi):
    return ar * br + ai * bi, ar * bi - ai * br


def masks(pos, p):
    row = pos[p, 0]
    col = pos[p, 1]
    i = lax.broadcasted_iota(jnp.int32, (HALF, HALF), 0)
    j = lax.broadcasted_iota(jnp.int32, (HALF, HALF), 1)
    flip = jnp.full((HALF, HALF), pos[2, 1]) == 1
    low = jnp.full((HALF, HALF), pos[2, 0]) == 1
    return i >= row, i + HALF >= row, (j >= col) == flip, low


def pick_rows(low, a, b):
    return jnp.where(low, a, b), jnp.where(low, b, a)


def window(own, cols_a, cols_b, rows_a, rows_b, pos, p, c):
    top, bottom, near, low = masks(pos, p)

    def band(k):
        return pick_rows(low, rows_a[c, :, k * HALF : (k + 1) * HALF], rows_b[c, :, k * HALF : (k + 1) * HALF])

    (up_a, down_a), (up, down), (up_b, down_b) = (band(0), band(1), band(2))
    side_u = jnp.where(near, up_a, up_b)
    side_d = jnp.where(near, down_a, down_b)
    side_t = jnp.where(near, cols_a[c, :HALF], cols_b[c, :HALF])
    side_l = jnp.where(near, cols_a[c, HALF:], cols_b[c, HALF:])
    side = cat([jnp.where(top, side_u, side_l), jnp.where(bottom, side_t, side_d)], 0)
    mid = cat([jnp.where(top, up, own[c, HALF:, :]), jnp.where(bottom, own[c, :HALF, :], down)], 0)
    return cat([side, mid], 1)


def put_gradient(g0, g1, c, pos, own, cols_a, cols_b, rows_a, rows_b):
    def pieces(g, p):
        top, bottom, near, _ = masks(pos, p)
        zero = jnp.zeros((HALF, HALF), f32)
        out = []
        for rows, keep in ((g[:HALF], top), (g[HALF:], bottom)):
            for inside in (keep, jnp.logical_not(keep)):
                side = jnp.where(inside, rows[:, :HALF], zero)
                mid = jnp.where(inside, rows[:, HALF:], zero)
                out.append((jnp.where(near, side, zero), mid, jnp.where(near, zero, side)))
        return out

    low = masks(pos, 0)[3]
    u0, b0, t0, d0 = pieces(g0, 0)
    u1, b1, t1, d1 = pieces(g1, 1)
    for k in range(3):
        cols = slice(k * HALF, (k + 1) * HALF)
        first, second = pick_rows(low, u0[k] + u1[k], d0[k] + d1[k])
        rows_a[c, :, cols] = first
        rows_b[c, :, cols] = second
        part = (cols_a, own, cols_b)[k]
        part[c, :HALF, :] = t0[k] + t1[k]
        part[c, HALF:, :] = b0[k] + b1[k]


def prepare_kernel(pos, probe, phase, intensity, probe_out, trans_out, intensity_out):
    for p in range(2):
        row = pos[p, 0]
        col = pos[p, 1]
        for c in range(2):
            rolled = pltpu.roll(probe[c], row, 0)
            probe_out[p, c] = pltpu.roll(rolled, col, 1)
    i = lax.broadcasted_iota(jnp.int32, (N, N), 0)
    j = lax.broadcasted_iota(jnp.int32, (N, N), 1)
    source = jnp.where(j < HALF, 2 * j, 2 * (j - HALF) + 1)
    pick = jnp.where(i == source, 1.0, 0.0).astype(bf16)
    target = jnp.where(i < HALF, 2 * i, 2 * (i - HALF) + 1)
    pick_rows = jnp.where(j == target, 1.0, 0.0).astype(bf16)

    def thirds(x):
        hi = x.astype(bf16)
        rest = x - hi.astype(f32)
        mid = rest.astype(bf16)
        return hi, mid, (rest - mid.astype(f32)).astype(bf16)

    def reorder(x):
        x = sum(dot(pick_rows, part) for part in thirds(x))
        return sum(dot(part, pick) for part in thirds(x))

    ph = reorder(phase[...])
    trans_out[0] = jnp.cos(ph)
    trans_out[1] = jnp.sin(ph)
    for p in range(2):
        intensity_out[p] = reorder(intensity[p])


def exit_kernel(pos, own, cols_a, cols_b, rows_a, rows_b, probe, trans, tab, wave):
    for p in range(2):
        wr = window(own, cols_a, cols_b, rows_a, rows_b, pos, p, 0)
        wi = window(own, cols_a, cols_b, rows_a, rows_b, pos, p, 1)
        re, im = cmul(probe[p, 0], probe[p, 1], wr, wi)
        re, im = forward(tab, re, im)
        re, im = cmul(trans[0], trans[1], re, im)
        re, im = inverse(tab, re, im)
        wave[p, 0] = re
        wave[p, 1] = im


def far_kernel(pos, own, cols_a, cols_b, rows_a, rows_b, wave, intensity, tab, back, g_own, g_cols_a, g_cols_b, g_rows_a, g_rows_b):
    grads = []
    for p in range(2):
        wr = window(own, cols_a, cols_b, rows_a, rows_b, pos, p, 0)
        wi = window(own, cols_a, cols_b, rows_a, rows_b, pos, p, 1)
        re, im = cmul(wave[p, 0], wave[p, 1], wr, wi)
        re, im = forward(tab, re, im)
        scale = 2.0 * (re * re + im * im - intensity[p])
        re, im = inverse(tab, scale * re, scale * im)
        br, bi = cmul_conj(wr, wi, re, im)
        back[p, 0] = br
        back[p, 1] = bi
        grads.append(cmul_conj(wave[p, 0], wave[p, 1], re, im))
    for c in range(2):
        put_gradient(grads[0][c], grads[1][c], c, pos, g_own, g_cols_a, g_cols_b, g_rows_a, g_rows_b)


def first_kernel(pos, back, probe, trans, tab, g_own, g_cols_a, g_cols_b, g_rows_a, g_rows_b):
    grads = []
    for p in range(2):
        re, im = forward(tab, back[p, 0], back[p, 1])
        re, im = cmul_conj(trans[0], trans[1], re, im)
        re, im = inverse(tab, re, im)
        grads.append(cmul_conj(probe[p, 0], probe[p, 1], re, im))
    for c in range(2):
        put_gradient(grads[0][c], grads[1][c], c, pos, g_own, g_cols_a, g_cols_b, g_rows_a, g_rows_b)


def merge_kernel(pos, own, cols_a, cols_b, rows_a, rows_b, sum_own, send_a, send_b):
    low = masks(pos, 0)[3]
    for c in range(2):
        for k, (part, out) in enumerate(((cols_a, send_a), (own, sum_own), (cols_b, send_b))):
            cols = slice(k * HALF, (k + 1) * HALF)
            top, bottom = pick_rows(low, rows_a[c, :, cols], rows_b[c, :, cols])
            out[c, :HALF, :] = part[c, :HALF, :] + top
            out[c, HALF:, :] = part[c, HALF:, :] + bottom


def second_update_kernel(
    pos, own, from_a, from_b, objects, momentum, object_next, momentum_next, base_o, base_m, old_o, old_m, new_o, new_m, sems
):
    loads = [
        pltpu.make_async_copy(objects, old_o, sems.at[0]),
        pltpu.make_async_copy(momentum, old_m, sems.at[1]),
    ]
    for copy in loads:
        copy.start()
    for copy in loads:
        copy.wait()
    keep = decay_rate * old_m[0]
    base_m[...] = keep
    base_o[...] = old_o[0] - step_length * keep
    m = decay_rate * old_m[1] + grad_scale * (own[...] + from_a[...] + from_b[...])
    new_m[...] = m
    new_o[...] = old_o[1] - step_length * m
    stores = [
        pltpu.make_async_copy(new_o, object_next.at[1], sems.at[0]),
        pltpu.make_async_copy(new_m, momentum_next.at[1], sems.at[1]),
    ]
    for copy in stores:
        copy.start()
    for copy in stores:
        copy.wait()


def first_update_kernel(
    pos, own, from_a, from_b, base_o, base_m, object_in, momentum_in, object_next, momentum_next, new_o, new_m, sems
):
    g = grad_scale * (own[...] + from_a[...] + from_b[...])
    new_m[...] = base_m[...] + g
    new_o[...] = base_o[...] - step_length * g
    stores = [
        pltpu.make_async_copy(new_o, object_next.at[0], sems.at[0]),
        pltpu.make_async_copy(new_m, momentum_next.at[0], sems.at[1]),
    ]
    for copy in stores:
        copy.start()
    for copy in stores:
        copy.wait()


VMEM = pl.BlockSpec(memory_space=pltpu.VMEM)
ANY = pl.BlockSpec(memory_space=pl.ANY)
HBM = pl.BlockSpec(memory_space=pltpu.HBM)
TILE = (2, 256, 128)
FULL = (2, 2, 256, 128)


def second_update(pos, own, from_a, from_b, objects, momentum):
    shapes = (FULL, FULL, TILE, TILE)
    scratch = [pltpu.VMEM(FULL, f32)] * 2 + [pltpu.VMEM(TILE, f32)] * 2 + [pltpu.SemaphoreType.DMA((2,))]
    return pl.pallas_call(
        second_update_kernel,
        out_shape=[jax.ShapeDtypeStruct(x, f32) for x in shapes],
        in_specs=[pl.BlockSpec(memory_space=pltpu.SMEM)] + [VMEM] * 3 + [HBM] * 2,
        out_specs=[HBM, HBM, VMEM, VMEM],
        scratch_shapes=scratch,
        compiler_params=pltpu.CompilerParams(vmem_limit_bytes=8 * 2**20),
        cost_estimate=pl.CostEstimate(flops=10**9, bytes_accessed=2**21, transcendentals=0),
        name="second_update",
    )(pos, own, from_a, from_b, objects, momentum)


def first_update(pos, own, from_a, from_b, base_o, base_m, object_next, momentum_next):
    return pl.pallas_call(
        first_update_kernel,
        out_shape=[jax.ShapeDtypeStruct(FULL, f32)] * 2,
        in_specs=[pl.BlockSpec(memory_space=pltpu.SMEM)] + [VMEM] * 5 + [HBM] * 2,
        out_specs=[HBM] * 2,
        scratch_shapes=[pltpu.VMEM(TILE, f32)] * 2 + [pltpu.SemaphoreType.DMA((2,))],
        input_output_aliases={6: 0, 7: 1},
        compiler_params=pltpu.CompilerParams(vmem_limit_bytes=8 * 2**20),
        cost_estimate=pl.CostEstimate(flops=10**9, bytes_accessed=2**21, transcendentals=0),
        name="first_update",
    )(pos, own, from_a, from_b, base_o, base_m, object_next, momentum_next)


def call(kernel, outs, args, flops):
    specs = [pl.BlockSpec(memory_space=pltpu.SMEM)] + [pl.BlockSpec(memory_space=pltpu.VMEM)] * (len(args) - 1)
    return pl.pallas_call(
        kernel,
        out_shape=[jax.ShapeDtypeStruct(s, f32) for s in outs],
        in_specs=specs,
        out_specs=[pl.BlockSpec(memory_space=pltpu.VMEM)] * len(outs),
        compiler_params=pltpu.CompilerParams(vmem_limit_bytes=20 * 2**20),
        cost_estimate=pl.CostEstimate(flops=flops, bytes_accessed=4 * 2**20, transcendentals=0),
    )(*args)


GRAD_SHAPES = ((2, 256, 128),) * 3 + ((2, 128, 384),) * 2


def swap(value, axis, first):
    count = lax.axis_size(axis)
    there = [(k, k + 1) for k in range(first, count - 1, 2)]
    return lax.ppermute(value, axis, there + [(b, a) for a, b in there])


def halos(tile, low):
    cols_b = swap(tile, "tx", 1)
    cols_a = swap(tile, "tx", 0)
    band = cat([cols_a, tile, cols_b], 2)
    top, bottom = (band[:, :HALF], band[:, HALF:])
    rows_b = swap(jnp.where(low, bottom, top), "ty", 1)
    rows_a = swap(jnp.where(low, top, bottom), "ty", 0)
    return tile, cols_a, cols_b, rows_a, rows_b


def gather_gradient(pos, own, cols_a, cols_b, rows_a, rows_b):
    rows_b = swap(rows_b, "ty", 1)
    rows_a = swap(rows_a, "ty", 0)
    own, send_a, send_b = call(merge_kernel, (TILE,) * 3, (pos, own, cols_a, cols_b, rows_a, rows_b), 10**8)
    from_b = swap(send_b, "tx", 1)
    from_a = swap(send_a, "tx", 0)
    return own, from_a, from_b


def on_device(intensity, corner, probe, prop_phase, object_slices, momentum):
    tile_rows, tile_cols = object_slices.shape[2:]
    at_y, at_x = (lax.axis_index("ty"), lax.axis_index("tx"))
    origin = jnp.stack([at_y * tile_rows - HALF, at_x * tile_cols - HALF])
    parity = jnp.stack([at_y % 2, at_x % 2])
    pos = jnp.concatenate([corner - origin[None, :], parity[None, :]])
    low = at_y % 2 == 1
    tab = jnp.asarray(dft_tables())
    first = halos(object_slices[0], low)
    second = halos(object_slices[1], low)
    probe_r, trans, inten = call(
        prepare_kernel, ((2, 2, N, N), (2, N, N), (2, N, N)), (pos, probe, prop_phase, intensity), 2 * 10**9
    )
    (wave,) = call(exit_kernel, ((2, 2, N, N),), (pos, *first, probe_r, trans, tab), 4 * 10**9)
    back, *g2 = call(far_kernel, ((2, 2, N, N),) + GRAD_SHAPES, (pos, *second, wave, inten, tab), 4 * 10**9)
    g1 = call(first_kernel, GRAD_SHAPES, (pos, back, probe_r, trans, tab), 4 * 10**9)
    grad_second = gather_gradient(pos, *g2)
    grad_first = gather_gradient(pos, *g1)
    object_next, momentum_next, base_o, base_m = second_update(pos, *grad_second, object_slices, momentum)
    out = first_update(pos, *grad_first, base_o, base_m, object_next, momentum_next)
    return tuple(out)


def solution(mesh):
    return jax.shard_map(
        on_device,
        mesh=mesh,
        in_specs=(
            P(("ty", "tx"), None, None),
            P(("ty", "tx"), None),
            P(),
            P(),
            P(None, None, "ty", "tx"),
            P(None, None, "ty", "tx"),
        ),
        out_specs=(P(None, None, "ty", "tx"), P(None, None, "ty", "tx")),
        check_vma=False,
    )
```

```python
import math

import jax
import jax.numpy as jnp
import numpy as np
from jax import lax
from jax.experimental import pallas as pl
from jax.experimental.pallas import tpu as pltpu
from jax.sharding import PartitionSpec as P


decay_rate = 0.9
grad_scale = 0.05
step_length = 0.5

N = 256
HALF = 128
bf16 = jnp.bfloat16
f32 = jnp.float32


def dft_tables():
    j = np.arange(HALF)[:, None]
    k = np.arange(HALF)[None, :]
    even = np.exp(-2j * math.pi * (j * (2 * k) % N) / N) / math.sqrt(N)
    odd = np.exp(-2j * math.pi * (j * (2 * k + 1) % N) / N) / math.sqrt(N)
    out = []
    for m in (even, odd):
        real = np.block([[m.real, m.imag], [-m.imag, m.real]])
        for t in (real, real.T):
            t = t.astype(np.float32)
            hi = t.astype(jnp.bfloat16)
            lo = (t - hi.astype(np.float32)).astype(jnp.bfloat16)
            out += [hi, lo]
    return np.stack(out)


EVEN, EVEN_T, ODD, ODD_T = (0, 2, 4, 6)


def split(x):
    hi = x.astype(bf16)
    lo = (x - hi.astype(f32)).astype(bf16)
    return hi, lo


def dot(a, b):
    return jnp.dot(a, b, preferred_element_type=f32)


def left_mul(tab, which, x):
    hi, lo = split(x)
    return dot(tab[which], hi) + dot(tab[which], lo) + dot(tab[which + 1], hi)


def right_mul(tab, which, x):
    hi, lo = split(x)
    return dot(hi, tab[which]) + dot(lo, tab[which]) + dot(hi, tab[which + 1])


def cat(parts, axis):
    return jnp.concatenate(parts, axis=axis)


def forward(tab, re, im):
    a = cat([re[:HALF] + re[HALF:], im[:HALF] + im[HALF:]], 0)
    b = cat([re[:HALF] - re[HALF:], im[:HALF] - im[HALF:]], 0)
    e = left_mul(tab, EVEN_T, a)
    o = left_mul(tab, ODD_T, b)
    re = cat([e[:HALF], o[:HALF]], 0)
    im = cat([e[HALF:], o[HALF:]], 0)
    a = cat([re[:, :HALF] + re[:, HALF:], im[:, :HALF] + im[:, HALF:]], 1)
    b = cat([re[:, :HALF] - re[:, HALF:], im[:, :HALF] - im[:, HALF:]], 1)
    e = right_mul(tab, EVEN, a)
    o = right_mul(tab, ODD, b)
    re = cat([e[:, :HALF], o[:, :HALF]], 1)
    im = cat([e[:, HALF:], o[:, HALF:]], 1)
    return re, im


def inverse(tab, re, im):
    e = right_mul(tab, EVEN_T, cat([re[:, :HALF], im[:, :HALF]], 1))
    o = right_mul(tab, ODD_T, cat([re[:, HALF:], im[:, HALF:]], 1))
    s, d = e + o, e - o
    re = cat([s[:, :HALF], d[:, :HALF]], 1)
    im = cat([s[:, HALF:], d[:, HALF:]], 1)
    e = left_mul(tab, EVEN, cat([re[:HALF], im[:HALF]], 0))
    o = left_mul(tab, ODD, cat([re[HALF:], im[HALF:]], 0))
    s, d = e + o, e - o
    re = cat([s[:HALF], d[:HALF]], 0)
    im = cat([s[HALF:], d[HALF:]], 0)
    return re, im


def cmul(ar, ai, br, bi):
    return ar * br - ai * bi, ar * bi + ai * br


def cmul_conj(ar, ai, br, bi):
    return ar * br + ai * bi, ar * bi - ai * br


def masks(pos, p):
    row = pos[p, 0]
    col = pos[p, 1]
    i = lax.broadcasted_iota(jnp.int32, (HALF, HALF), 0)
    j = lax.broadcasted_iota(jnp.int32, (HALF, HALF), 1)
    flip = jnp.full((HALF, HALF), pos[2, 1]) == 1
    low = jnp.full((HALF, HALF), pos[2, 0]) == 1
    return i >= row, i + HALF >= row, (j >= col) == flip, low


def pick_rows(low, a, b):
    return jnp.where(low, a, b), jnp.where(low, b, a)


def window(own, cols_a, cols_b, rows_a, rows_b, pos, p, c):
    top, bottom, near, low = masks(pos, p)

    def band(k):
        return pick_rows(low, rows_a[c, :, k * HALF : (k + 1) * HALF], rows_b[c, :, k * HALF : (k + 1) * HALF])

    (up_a, down_a), (up, down), (up_b, down_b) = (band(0), band(1), band(2))
    side_u = jnp.where(near, up_a, up_b)
    side_d = jnp.where(near, down_a, down_b)
    side_t = jnp.where(near, cols_a[c, :HALF], cols_b[c, :HALF])
    side_l = jnp.where(near, cols_a[c, HALF:], cols_b[c, HALF:])
    side = cat([jnp.where(top, side_u, side_l), jnp.where(bottom, side_t, side_d)], 0)
    mid = cat([jnp.where(top, up, own[c, HALF:, :]), jnp.where(bottom, own[c, :HALF, :], down)], 0)
    return cat([side, mid], 1)


def put_gradient(g0, g1, c, pos, own, cols_a, cols_b, rows_a, rows_b):
    def pieces(g, p):
        top, bottom, near, _ = masks(pos, p)
        zero = jnp.zeros((HALF, HALF), f32)
        out = []
        for rows, keep in ((g[:HALF], top), (g[HALF:], bottom)):
            for inside in (keep, jnp.logical_not(keep)):
                side = jnp.where(inside, rows[:, :HALF], zero)
                mid = jnp.where(inside, rows[:, HALF:], zero)
                out.append((jnp.where(near, side, zero), mid, jnp.where(near, zero, side)))
        return out

    low = masks(pos, 0)[3]
    u0, b0, t0, d0 = pieces(g0, 0)
    u1, b1, t1, d1 = pieces(g1, 1)
    for k in range(3):
        cols = slice(k * HALF, (k + 1) * HALF)
        first, second = pick_rows(low, u0[k] + u1[k], d0[k] + d1[k])
        rows_a[c, :, cols] = first
        rows_b[c, :, cols] = second
        part = (cols_a, own, cols_b)[k]
        part[c, :HALF, :] = t0[k] + t1[k]
        part[c, HALF:, :] = b0[k] + b1[k]


def prepare_kernel(pos, probe, phase, intensity, probe_out, trans_out, intensity_out):
    for p in range(2):
        row = pos[p, 0]
        col = pos[p, 1]
        for c in range(2):
            rolled = pltpu.roll(probe[c], row, 0)
            probe_out[p, c] = pltpu.roll(rolled, col, 1)
    i = lax.broadcasted_iota(jnp.int32, (N, N), 0)
    j = lax.broadcasted_iota(jnp.int32, (N, N), 1)
    source = jnp.where(j < HALF, 2 * j, 2 * (j - HALF) + 1)
    pick = jnp.where(i == source, 1.0, 0.0).astype(bf16)
    target = jnp.where(i < HALF, 2 * i, 2 * (i - HALF) + 1)
    pick_rows = jnp.where(j == target, 1.0, 0.0).astype(bf16)

    def thirds(x):
        hi = x.astype(bf16)
        rest = x - hi.astype(f32)
        mid = rest.astype(bf16)
        return hi, mid, (rest - mid.astype(f32)).astype(bf16)

    def reorder(x):
        x = sum(dot(pick_rows, part) for part in thirds(x))
        return sum(dot(part, pick) for part in thirds(x))

    ph = reorder(phase[...])
    trans_out[0] = jnp.cos(ph)
    trans_out[1] = jnp.sin(ph)
    for p in range(2):
        intensity_out[p] = reorder(intensity[p])


def exit_kernel(pos, own, cols_a, cols_b, rows_a, rows_b, probe, trans, tab, wave):
    for p in range(2):
        wr = window(own, cols_a, cols_b, rows_a, rows_b, pos, p, 0)
        wi = window(own, cols_a, cols_b, rows_a, rows_b, pos, p, 1)
        re, im = cmul(probe[p, 0], probe[p, 1], wr, wi)
        re, im = forward(tab, re, im)
        re, im = cmul(trans[0], trans[1], re, im)
        re, im = inverse(tab, re, im)
        wave[p, 0] = re
        wave[p, 1] = im


def far_kernel(pos, own, cols_a, cols_b, rows_a, rows_b, wave, intensity, tab, back, g_own, g_cols_a, g_cols_b, g_rows_a, g_rows_b):
    grads = []
    for p in range(2):
        wr = window(own, cols_a, cols_b, rows_a, rows_b, pos, p, 0)
        wi = window(own, cols_a, cols_b, rows_a, rows_b, pos, p, 1)
        re, im = cmul(wave[p, 0], wave[p, 1], wr, wi)
        re, im = forward(tab, re, im)
        scale = 2.0 * (re * re + im * im - intensity[p])
        re, im = inverse(tab, scale * re, scale * im)
        br, bi = cmul_conj(wr, wi, re, im)
        back[p, 0] = br
        back[p, 1] = bi
        grads.append(cmul_conj(wave[p, 0], wave[p, 1], re, im))
    for c in range(2):
        put_gradient(grads[0][c], grads[1][c], c, pos, g_own, g_cols_a, g_cols_b, g_rows_a, g_rows_b)


def first_kernel(pos, back, probe, trans, tab, g_own, g_cols_a, g_cols_b, g_rows_a, g_rows_b):
    grads = []
    for p in range(2):
        re, im = forward(tab, back[p, 0], back[p, 1])
        re, im = cmul_conj(trans[0], trans[1], re, im)
        re, im = inverse(tab, re, im)
        grads.append(cmul_conj(probe[p, 0], probe[p, 1], re, im))
    for c in range(2):
        put_gradient(grads[0][c], grads[1][c], c, pos, g_own, g_cols_a, g_cols_b, g_rows_a, g_rows_b)


def call(kernel, outs, args, flops):
    specs = [pl.BlockSpec(memory_space=pltpu.SMEM)] + [pl.BlockSpec(memory_space=pltpu.VMEM)] * (len(args) - 1)
    return pl.pallas_call(
        kernel,
        out_shape=[jax.ShapeDtypeStruct(s, f32) for s in outs],
        in_specs=specs,
        out_specs=[pl.BlockSpec(memory_space=pltpu.VMEM)] * len(outs),
        compiler_params=pltpu.CompilerParams(vmem_limit_bytes=20 * 2**20),
        cost_estimate=pl.CostEstimate(flops=flops, bytes_accessed=4 * 2**20, transcendentals=0),
    )(*args)


GRAD_SHAPES = ((2, 256, 128),) * 3 + ((2, 128, 384),) * 2


def swap(value, axis, first):
    rows, cols = (lax.axis_size("ty"), lax.axis_size("tx"))
    partner = {}
    for y in range(rows):
        for x in range(cols):
            if axis == "ty":
                other = ((y - first) ^ 1) + first
                partner[y, x] = (other % rows, x)
            else:
                other = ((x - first) ^ 1) + first
                partner[y, x] = (y, other) if 0 <= other < cols else (y ^ 1, x)
    pairs = [(y * cols + x, b * cols + a) for (y, x), (b, a) in partner.items()]
    return lax.ppermute(value, ("ty", "tx"), pairs)


def halos(tile, low):
    cols_b = swap(tile, "tx", 1)
    cols_a = swap(tile, "tx", 0)
    band = cat([cols_a, tile, cols_b], 2)
    top, bottom = (band[:, :HALF], band[:, HALF:])
    rows_b = swap(jnp.where(low, bottom, top), "ty", 1)
    rows_a = swap(jnp.where(low, top, bottom), "ty", 0)
    return tile, cols_a, cols_b, rows_a, rows_b


def gather_gradient(low, own, cols_a, cols_b, rows_a, rows_b):
    rows_b = swap(rows_b, "ty", 1)
    rows_a = swap(rows_a, "ty", 0)

    def merged(part, k):
        cols = slice(k * HALF, (k + 1) * HALF)
        first, second = (rows_a[:, :, cols], rows_b[:, :, cols])
        rows = cat([jnp.where(low, first, second), jnp.where(low, second, first)], 1)
        return part + rows

    send_a, send_b, own = merged(cols_a, 0), merged(cols_b, 2), merged(own, 1)
    from_b = swap(send_b, "tx", 1)
    from_a = swap(send_a, "tx", 0)
    return own, from_a, from_b


def on_device(intensity, corner, probe, prop_phase, object_slices, momentum):
    tile_rows, tile_cols = object_slices.shape[2:]
    at_y, at_x = (lax.axis_index("ty"), lax.axis_index("tx"))
    origin = jnp.stack([at_y * tile_rows - HALF, at_x * tile_cols - HALF])
    parity = jnp.stack([at_y % 2, at_x % 2])
    pos = jnp.concatenate([corner - origin[None, :], parity[None, :]])
    low = at_y % 2 == 1
    tab = jnp.asarray(dft_tables())
    tile1, rest = lax.optimization_barrier((object_slices[0], object_slices))
    first = halos(tile1, low)
    second = halos(rest[1], low)
    probe_r, trans, inten = call(
        prepare_kernel, ((2, 2, N, N), (2, N, N), (2, N, N)), (pos, probe, prop_phase, intensity), 2 * 10**9
    )
    (wave,) = call(exit_kernel, ((2, 2, N, N),), (pos, *first, probe_r, trans, tab), 4 * 10**9)
    back, *g2 = call(far_kernel, ((2, 2, N, N),) + GRAD_SHAPES, (pos, *second, wave, inten, tab), 4 * 10**9)
    g1 = call(first_kernel, GRAD_SHAPES, (pos, back, probe_r, trans, tab), 4 * 10**9)
    grad_second = gather_gradient(low, *g2)
    grad_first = gather_gradient(low, *g1)
    keep = decay_rate * momentum
    rest = object_slices - step_length * keep
    keep, rest = lax.optimization_barrier((keep, rest))
    gradient = grad_scale * jnp.stack([sum(grad_first), sum(grad_second)])
    momentum_next = keep + gradient
    object_next = rest - step_length * gradient
    return (object_next, momentum_next)


def solution(mesh):
    return jax.shard_map(
        on_device,
        mesh=mesh,
        in_specs=(
            P(("ty", "tx"), None, None),
            P(("ty", "tx"), None),
            P(),
            P(),
            P(None, None, "ty", "tx"),
            P(None, None, "ty", "tx"),
        ),
        out_specs=(P(None, None, "ty", "tx"), P(None, None, "ty", "tx")),
        check_vma=False,
    )
```

```python
import math

import jax
import jax.numpy as jnp
import numpy as np
from jax import lax
from jax.experimental import pallas as pl
from jax.experimental.pallas import tpu as pltpu
from jax.sharding import PartitionSpec as P


decay_rate = 0.9
grad_scale = 0.05
step_length = 0.5

N = 256
HALF = 128
bf16 = jnp.bfloat16
f32 = jnp.float32


def dft_tables():
    j = np.arange(HALF)[:, None]
    k = np.arange(HALF)[None, :]
    even = np.exp(-2j * math.pi * (j * (2 * k) % N) / N) / math.sqrt(N)
    odd = np.exp(-2j * math.pi * (j * (2 * k + 1) % N) / N) / math.sqrt(N)
    out = []
    for m in (even, odd):
        real = np.block([[m.real, m.imag], [-m.imag, m.real]])
        for t in (real, real.T):
            t = t.astype(np.float32)
            hi = t.astype(jnp.bfloat16)
            lo = (t - hi.astype(np.float32)).astype(jnp.bfloat16)
            out += [hi, lo]
    return np.stack(out)


EVEN, EVEN_T, ODD, ODD_T = (0, 2, 4, 6)


def split(x):
    hi = x.astype(bf16)
    lo = (x - hi.astype(f32)).astype(bf16)
    return hi, lo


def dot(a, b):
    return jnp.dot(a, b, preferred_element_type=f32)


def left_mul(tab, which, x):
    hi, lo = split(x)
    return dot(tab[which], hi) + dot(tab[which], lo) + dot(tab[which + 1], hi)


def right_mul(tab, which, x):
    hi, lo = split(x)
    return dot(hi, tab[which]) + dot(lo, tab[which]) + dot(hi, tab[which + 1])


def cat(parts, axis):
    return jnp.concatenate(parts, axis=axis)


def forward(tab, re, im):
    a = cat([re[:HALF] + re[HALF:], im[:HALF] + im[HALF:]], 0)
    b = cat([re[:HALF] - re[HALF:], im[:HALF] - im[HALF:]], 0)
    e = left_mul(tab, EVEN_T, a)
    o = left_mul(tab, ODD_T, b)
    re = cat([e[:HALF], o[:HALF]], 0)
    im = cat([e[HALF:], o[HALF:]], 0)
    a = cat([re[:, :HALF] + re[:, HALF:], im[:, :HALF] + im[:, HALF:]], 1)
    b = cat([re[:, :HALF] - re[:, HALF:], im[:, :HALF] - im[:, HALF:]], 1)
    e = right_mul(tab, EVEN, a)
    o = right_mul(tab, ODD, b)
    re = cat([e[:, :HALF], o[:, :HALF]], 1)
    im = cat([e[:, HALF:], o[:, HALF:]], 1)
    return re, im


def inverse(tab, re, im):
    e = right_mul(tab, EVEN_T, cat([re[:, :HALF], im[:, :HALF]], 1))
    o = right_mul(tab, ODD_T, cat([re[:, HALF:], im[:, HALF:]], 1))
    s, d = e + o, e - o
    re = cat([s[:, :HALF], d[:, :HALF]], 1)
    im = cat([s[:, HALF:], d[:, HALF:]], 1)
    e = left_mul(tab, EVEN, cat([re[:HALF], im[:HALF]], 0))
    o = left_mul(tab, ODD, cat([re[HALF:], im[HALF:]], 0))
    s, d = e + o, e - o
    re = cat([s[:HALF], d[:HALF]], 0)
    im = cat([s[HALF:], d[HALF:]], 0)
    return re, im


def cmul(ar, ai, br, bi):
    return ar * br - ai * bi, ar * bi + ai * br


def cmul_conj(ar, ai, br, bi):
    return ar * br + ai * bi, ar * bi - ai * br


def masks(pos, p):
    row = pos[p, 0]
    col = pos[p, 1]
    i = lax.broadcasted_iota(jnp.int32, (HALF, HALF), 0)
    j = lax.broadcasted_iota(jnp.int32, (HALF, HALF), 1)
    flip = jnp.full((HALF, HALF), pos[2, 1]) == 1
    low = jnp.full((HALF, HALF), pos[2, 0]) == 1
    return i >= row, i + HALF >= row, (j >= col) == flip, low


def pick_rows(low, a, b):
    return jnp.where(low, a, b), jnp.where(low, b, a)


def window(own, cols_a, cols_b, cor_a, cor_b, cen_a, cen_b, pos, p, c, first):
    top, bottom, near, low = masks(pos, p)
    up_a, down_a = pick_rows(low, cor_a[c, :, :HALF], cor_b[c, :, :HALF])
    up_b, down_b = pick_rows(low, cor_a[c, :, HALF:], cor_b[c, :, HALF:])
    up, down = pick_rows(low, cen_a[first + c], cen_b[first + c])
    side_u = jnp.where(near, up_a, up_b)
    side_d = jnp.where(near, down_a, down_b)
    side_t = jnp.where(near, cols_a[c, :HALF], cols_b[c, :HALF])
    side_l = jnp.where(near, cols_a[c, HALF:], cols_b[c, HALF:])
    side = cat([jnp.where(top, side_u, side_l), jnp.where(bottom, side_t, side_d)], 0)
    mid = cat([jnp.where(top, up, own[c, HALF:, :]), jnp.where(bottom, own[c, :HALF, :], down)], 0)
    return cat([side, mid], 1)


def put_gradient(g0, g1, c, pos, own, cols_a, cols_b, cor_a, cor_b, cen_a, cen_b):
    def pieces(g, p):
        top, bottom, near, _ = masks(pos, p)
        zero = jnp.zeros((HALF, HALF), f32)
        out = []
        for rows, keep in ((g[:HALF], top), (g[HALF:], bottom)):
            for inside in (keep, jnp.logical_not(keep)):
                side = jnp.where(inside, rows[:, :HALF], zero)
                mid = jnp.where(inside, rows[:, HALF:], zero)
                out.append((jnp.where(near, side, zero), mid, jnp.where(near, zero, side)))
        return out

    low = masks(pos, 0)[3]
    u0, b0, t0, d0 = pieces(g0, 0)
    u1, b1, t1, d1 = pieces(g1, 1)
    for k in range(3):
        first, second = pick_rows(low, u0[k] + u1[k], d0[k] + d1[k])
        if k == 1:
            cen_a[c] = first
            cen_b[c] = second
        else:
            cols = slice(0, HALF) if k == 0 else slice(HALF, N)
            cor_a[c, :, cols] = first
            cor_b[c, :, cols] = second
        part = (cols_a, own, cols_b)[k]
        part[c, :HALF, :] = t0[k] + t1[k]
        part[c, HALF:, :] = b0[k] + b1[k]


def prepare_kernel(pos, probe, phase, intensity, probe_out, trans_out, intensity_out):
    for p in range(2):
        row = pos[p, 0]
        col = pos[p, 1]
        for c in range(2):
            rolled = pltpu.roll(probe[c], row, 0)
            probe_out[p, c] = pltpu.roll(rolled, col, 1)
    i = lax.broadcasted_iota(jnp.int32, (N, N), 0)
    j = lax.broadcasted_iota(jnp.int32, (N, N), 1)
    source = jnp.where(j < HALF, 2 * j, 2 * (j - HALF) + 1)
    pick = jnp.where(i == source, 1.0, 0.0).astype(bf16)
    target = jnp.where(i < HALF, 2 * i, 2 * (i - HALF) + 1)
    pick_rows = jnp.where(j == target, 1.0, 0.0).astype(bf16)

    def thirds(x):
        hi = x.astype(bf16)
        rest = x - hi.astype(f32)
        mid = rest.astype(bf16)
        return hi, mid, (rest - mid.astype(f32)).astype(bf16)

    def reorder(x):
        x = sum(dot(pick_rows, part) for part in thirds(x))
        return sum(dot(part, pick) for part in thirds(x))

    ph = reorder(phase[...])
    trans_out[0] = jnp.cos(ph)
    trans_out[1] = jnp.sin(ph)
    for p in range(2):
        intensity_out[p] = reorder(intensity[p])


def exit_kernel(pos, own, cols_a, cols_b, cor_a, cor_b, cen_a, cen_b, probe, trans, tab, wave):
    for p in range(2):
        wr, wi = (window(own, cols_a, cols_b, cor_a, cor_b, cen_a, cen_b, pos, p, c, 0) for c in range(2))
        re, im = cmul(probe[p, 0], probe[p, 1], wr, wi)
        re, im = forward(tab, re, im)
        re, im = cmul(trans[0], trans[1], re, im)
        re, im = inverse(tab, re, im)
        wave[p, 0] = re
        wave[p, 1] = im


def far_kernel(pos, own, cols_a, cols_b, cor_a, cor_b, cen_a, cen_b, wave, intensity, tab, back, *outs):
    grads = []
    for p in range(2):
        wr, wi = (window(own, cols_a, cols_b, cor_a, cor_b, cen_a, cen_b, pos, p, c, 2) for c in range(2))
        re, im = cmul(wave[p, 0], wave[p, 1], wr, wi)
        re, im = forward(tab, re, im)
        scale = 2.0 * (re * re + im * im - intensity[p])
        re, im = inverse(tab, scale * re, scale * im)
        br, bi = cmul_conj(wr, wi, re, im)
        back[p, 0] = br
        back[p, 1] = bi
        grads.append(cmul_conj(wave[p, 0], wave[p, 1], re, im))
    for c in range(2):
        put_gradient(grads[0][c], grads[1][c], c, pos, *outs)


def first_kernel(pos, back, probe, trans, tab, *outs):
    grads = []
    for p in range(2):
        re, im = forward(tab, back[p, 0], back[p, 1])
        re, im = cmul_conj(trans[0], trans[1], re, im)
        re, im = inverse(tab, re, im)
        grads.append(cmul_conj(probe[p, 0], probe[p, 1], re, im))
    for c in range(2):
        put_gradient(grads[0][c], grads[1][c], c, pos, *outs)


def call(kernel, outs, args, flops):
    specs = [pl.BlockSpec(memory_space=pltpu.SMEM)] + [pl.BlockSpec(memory_space=pltpu.VMEM)] * (len(args) - 1)
    return pl.pallas_call(
        kernel,
        out_shape=[jax.ShapeDtypeStruct(s, f32) for s in outs],
        in_specs=specs,
        out_specs=[pl.BlockSpec(memory_space=pltpu.VMEM)] * len(outs),
        compiler_params=pltpu.CompilerParams(vmem_limit_bytes=20 * 2**20),
        cost_estimate=pl.CostEstimate(flops=flops, bytes_accessed=4 * 2**20, transcendentals=0),
    )(*args)


GRAD_SHAPES = ((2, 256, 128),) * 3 + ((2, 128, 256),) * 2 + ((2, 128, 128),) * 2


def swap(value, axis, first):
    rows, cols = (lax.axis_size("ty"), lax.axis_size("tx"))
    partner = {}
    for y in range(rows):
        for x in range(cols):
            if axis == "ty":
                other = ((y - first) ^ 1) + first
                partner[y, x] = (other % rows, x)
            else:
                other = ((x - first) ^ 1) + first
                partner[y, x] = (y, other) if 0 <= other < cols else (y ^ 1, x)
    pairs = [(y * cols + x, b * cols + a) for (y, x), (b, a) in partner.items()]
    return lax.ppermute(value, ("ty", "tx"), pairs)


def rows_exchange(to_a, to_b):
    rows_b = swap(to_b, "ty", 1)
    rows_a = swap(to_a, "ty", 0)
    return rows_a, rows_b


def facing(low, value):
    top, bottom = (value[:, :HALF], value[:, HALF:])
    return jnp.where(low, top, bottom), jnp.where(low, bottom, top)


def halos(tile, low):
    cols_b = swap(tile, "tx", 1)
    cols_a = swap(tile, "tx", 0)
    return tile, cols_a, cols_b, *rows_exchange(*facing(low, cat([cols_a, cols_b], 2)))


def stacked(low, rows_a, rows_b):
    return cat([jnp.where(low, rows_a, rows_b), jnp.where(low, rows_b, rows_a)], 1)


def gather_gradient(low, after, own, cols_a, cols_b, cor_a, cor_b):
    cor_a, cor_b = rows_exchange(cor_a, cor_b)
    cor_a, cor_b, *unused = lax.optimization_barrier((cor_a, cor_b, *after))
    rows = stacked(low, cor_a, cor_b)
    send_a, send_b = (cols_a + rows[:, :, :HALF], cols_b + rows[:, :, HALF:])
    from_b = swap(send_b, "tx", 1)
    from_a = swap(send_a, "tx", 0)
    return own + from_a + from_b, (send_a, send_b)


def on_device(intensity, corner, probe, prop_phase, object_slices, momentum):
    tile_rows, tile_cols = object_slices.shape[2:]
    at_y, at_x = (lax.axis_index("ty"), lax.axis_index("tx"))
    origin = jnp.stack([at_y * tile_rows - HALF, at_x * tile_cols - HALF])
    parity = jnp.stack([at_y % 2, at_x % 2])
    pos = jnp.concatenate([corner - origin[None, :], parity[None, :]])
    low = at_y % 2 == 1
    tab = jnp.asarray(dft_tables())
    first = halos(object_slices[0], low)
    second = halos(object_slices[1], low)
    planes = object_slices.reshape(4, tile_rows, tile_cols)
    centre = rows_exchange(*facing(low, planes))
    probe_r, trans, inten = call(
        prepare_kernel, ((2, 2, N, N), (2, N, N), (2, N, N)), (pos, probe, prop_phase, intensity), 2 * 10**9
    )
    (wave,) = call(exit_kernel, ((2, 2, N, N),), (pos, *first, *centre, probe_r, trans, tab), 4 * 10**9)
    back, *g2 = call(far_kernel, ((2, 2, N, N),) + GRAD_SHAPES, (pos, *second, *centre, wave, inten, tab), 4 * 10**9)
    g1 = call(first_kernel, GRAD_SHAPES, (pos, back, probe_r, trans, tab), 4 * 10**9)
    grad_second, sent = gather_gradient(low, (), *g2[:5])
    grad_first, sent = gather_gradient(low, sent, *g1[:5])
    cen = stacked(low, *rows_exchange(cat([g1[5], g2[5]], 0), cat([g1[6], g2[6]], 0)))
    keep = decay_rate * momentum
    rest = object_slices - step_length * keep
    keep, rest = lax.optimization_barrier((keep, rest))
    gradient = grad_scale * (cen.reshape(momentum.shape) + jnp.stack([grad_first, grad_second]))
    momentum_next = keep + gradient
    object_next = rest - step_length * gradient
    return (object_next, momentum_next)


def solution(mesh):
    return jax.shard_map(
        on_device,
        mesh=mesh,
        in_specs=(
            P(("ty", "tx"), None, None),
            P(("ty", "tx"), None),
            P(),
            P(),
            P(None, None, "ty", "tx"),
            P(None, None, "ty", "tx"),
        ),
        out_specs=(P(None, None, "ty", "tx"), P(None, None, "ty", "tx")),
        check_vma=False,
    )
```
